64 devices in a mesh: rep: 8 (over x, y, core), dp: 8 (over z).
Axes of the slice: x: 2, y: 2, z: 8, core: 2. Of those that a mesh axis runs over, the one named last changes fastest.
The devices are a block of a 4x4x8 slice.
Arguments:
- x: bfloat16 [64, 2048, 512], P(('rep', 'dp')), parts along dimension 0
- dy: bfloat16 [64, 2048, 512], P(('rep', 'dp')), parts along dimension 0
- w_gate: bfloat16 [2, 512, 1792], P(None, 'dp')
- w_up: bfloat16 [2, 512, 1792], P(None, 'dp')
- w_down: bfloat16 [2, 1792, 512], P(None, 'dp')
Outputs:
- output 1: bfloat16 [64, 2048, 512], P(('rep', 'dp')), parts along dimension 0
- output 2: bfloat16 [16, 512, 1792], P('rep', 'dp'), parts along dimension 0
- output 3: bfloat16 [16, 512, 1792], P('rep', 'dp'), parts along dimension 0
- output 4: bfloat16 [16, 1792, 512], P('rep', 'dp'), parts along dimension 0
There are 8 independent parts. The reference program is written for one: setup_inputs(seed, part) draws one part's arguments, and reference() takes and returns one part's arrays. A program takes and returns all parts, laid end to end along the dimension named above; an argument that names none is the same for every part.
All inputs are finite; a program needn't handle non-finite values.
Results may differ from the reference program's by a relative error of at most 0.018.
Values are sent between devices in bfloat16 or wider.
A program may use at most 768 MiB of HBM per device.

```python
import jax
import jax.numpy as jnp
from jax import lax

SEQUENCES = 8
TOKENS = 2048
D = 512
FF = 1792
LAYERS = 2
NAMES = ("w_gate", "w_up", "w_down")
SHAPES = {"w_gate": (LAYERS, D, FF), "w_up": (LAYERS, D, FF), "w_down": (LAYERS, FF, D)}


def bump(key, n, height):
    away = (jnp.arange(n, dtype=jnp.int32) - jax.random.randint(key, (), 0, n, jnp.int32)) % n
    return jnp.where(away < n // 8, height, 1.0)


def together(key, own, strength):
    shared = jax.random.normal(key, own.shape[1:], jnp.float32)
    return (own + strength * shared) * lax.rsqrt(1 + strength * strength)


def setup_inputs(seed: int = 0, part: int = 0) -> dict:
    kx, kdy, ka, kb, kz, kf, kh, kl, *kw = jax.random.split(jax.random.key(seed), 8 + len(NAMES))
    kx, kdy, ka, kb = (jax.random.fold_in(k, part) for k in (kx, kdy, ka, kb))
    shape = (SEQUENCES, TOKENS, D)
    much_x, much_dy = jax.random.uniform(kz, (2,), jnp.float32, 0.0, 1.0)
    layers = 2.0 ** jax.random.uniform(kl, (LAYERS, 1, 1), jnp.float32, -1.0, 1.0)
    x = together(ka, jax.random.normal(kx, shape, jnp.float32), much_x) * bump(kf, D, 4.0)
    dy = together(kb, jax.random.normal(kdy, shape, jnp.float32), much_dy)
    drawn = {"x": x.astype(jnp.bfloat16), "dy": (dy * (SEQUENCES * TOKENS) ** -0.5).astype(jnp.bfloat16)}
    for key, name in zip(kw, NAMES, strict=True):
        w = jax.random.normal(key, SHAPES[name], jnp.float32) * SHAPES[name][1] ** -0.5
        drawn[name] = (w * {"w_gate": 1.0, "w_up": bump(kh, FF, 4.0), "w_down": layers}[name]).astype(jnp.bfloat16)
    return drawn


def matmul(a, w):
    return jnp.dot(a, w, preferred_element_type=jnp.float32).astype(jnp.bfloat16)


def normed(h):
    wide = h.astype(jnp.float32)
    scale = lax.rsqrt(jnp.mean(wide**2, -1, keepdims=True) + 1e-6)
    return (wide * scale).astype(jnp.bfloat16)


def layer(h, w):
    a = normed(h)
    gate = jnp.dot(a, w["w_gate"], preferred_element_type=jnp.float32)
    up = jnp.dot(a, w["w_up"], preferred_element_type=jnp.float32)
    return h + matmul((jax.nn.silu(gate) * up).astype(jnp.bfloat16), w["w_down"])


def stack(weights, h):
    return lax.scan(lambda h, w: (layer(h, w), None), h, weights)[0]


def reference(x, dy, w_gate, w_up, w_down):
    weights = dict(zip(NAMES, (w_gate, w_up, w_down), strict=True))

    def take(so_far, sequence):
        h, by_y = sequence
        _, back = jax.vjp(stack, weights, h)
        by_weights, by_h = back(by_y)
        return jax.tree.map(lambda total, term: total + term.astype(jnp.float32), so_far, by_weights), by_h

    none_yet = {name: jnp.zeros(w.shape, jnp.float32) for name, w in weights.items()}
    by_weights, by_x = lax.scan(take, none_yet, (x, dy))
    return (by_x, *(by_weights[name].astype(jnp.bfloat16) for name in NAMES))
```

```python
import functools

import jax
import jax.numpy as jnp
from jax import lax
from jax.experimental import pallas as pl
from jax.experimental.pallas import tpu as pltpu
from jax.sharding import PartitionSpec as P

MESH = pl.DeviceIdType.MESH
F32, BF16 = jnp.float32, jnp.bfloat16
NN = (((1,), (0,)), ((), ()))
NT = (((1,), (1,)), ((), ()))


def dot(a, b, dims=NN):
    return lax.dot_general(a, b, dims, preferred_element_type=F32)


def chips_apart(mesh):
    first = mesh.devices.reshape(mesh.shape["rep"], -1)[:, 0]
    places = [getattr(d, "coords", None) for d in first]
    if places[0] is None:
        return 2, 4
    near = 2
    far = next((i for i, p in enumerate(places) if p[0] != places[0][0]), 4)
    return near, far


def kernel(cfg, x_hbm, dy_hbm, wp_hbm, dx_hbm, out_hbm,
           x, d, h, a, at, dt, acc, dgu, hid, w, g, ra, rb, out,
           zs, zr, xs, xr, cs, cr, rs, rr, local):
    n, near, far, tile, layers = cfg
    tokens, width = x.shape
    chunks, _, rows, _ = w.shape
    blocks = chunks // layers
    tall = width // n
    fb = width // 2
    quarter, half = width // 4, width // 2
    tiles = tokens // tile

    me, rep = lax.axis_index("dp"), lax.axis_index("rep")
    core, ybit, xbit = rep % 2, (rep // near) % 2, (rep // far) % 2
    other_core = rep + 1 - 2 * core
    other_y = rep + near * (1 - 2 * ybit)
    other_x = rep + far * (1 - 2 * xbit)

    def at_z(k):
        return lax.rem(me + k + 2 * n, n)

    barrier = pltpu.get_barrier_semaphore()
    for who in ({"dp": at_z(1)}, {"dp": at_z(-1)}, {"rep": other_core}, {"rep": other_y}, {"rep": other_x}):
        pl.semaphore_signal(barrier, inc=1, device_id=who, device_id_type=MESH)
    own = pltpu.make_async_copy(wp_hbm, w.at[:, me], local.at[0])
    own.start()
    get_x = pltpu.make_async_copy(x_hbm, x, local.at[1])
    get_x.start()
    get_d = pltpu.make_async_copy(dy_hbm, d, local.at[2])
    get_d.start()
    own.wait()
    pl.semaphore_wait(barrier, 5)

    def remote(src, dst, ssem, rsem, who):
        return pltpu.make_async_remote_copy(
            src_ref=src, dst_ref=dst, send_sem=ssem, recv_sem=rsem, device_id=who, device_id_type=MESH)

    def ag_chunk(c, k):
        par = c % 2
        s = 1 - 2 * par
        bit = ybit + par * (xbit - ybit)
        partner = other_y + par * (other_x - other_y)
        mine = pl.ds(pl.multiple_of((2 * core + bit) * quarter, quarter), quarter)
        theirs = pl.ds(pl.multiple_of((2 * core + 1 - bit) * quarter, quarter), quarter)
        mine2 = pl.ds(pl.multiple_of(core * half, half), half)
        theirs2 = pl.ds(pl.multiple_of((1 - core) * half, half), half)
        a_to, b_to = {"dp": at_z(s)}, {"dp": at_z(-s)}

        def hop(who, piece, m):
            ref = w.at[c, piece, :, mine]
            return remote(ref, ref, zs.at[c, m], zr.at[c, m], who)

        def across(piece, cols, m):
            ref = w.at[c, piece, :, cols]
            return remote(ref, ref, xs.at[c, m], xr.at[c, m], {"rep": partner})

        def within(piece, cols, m):
            ref = w.at[c, piece, :, cols]
            return remote(ref, ref, cs.at[c, m], cr.at[c, m], {"rep": other_core})

        def pieces(j):
            found = []
            if 1 <= j <= 4:
                found.append((at_z(-j * s), j - 1, a_to if j < 4 else None))
            if 1 <= j <= 3:
                found.append((at_z(j * s), 4 + j - 1, b_to if j < 3 else None))
            return found

        if k == 0:
            hop(a_to, me, 0).start()
            hop(b_to, me, 4).start()
        for piece, m, on in pieces(k):
            hop(a_to, piece, m).wait_recv()
            if on is not None:
                hop(on, piece, m + 1).start()
            across(piece, mine, m).start()
        for piece, m, _ in pieces(k - 1):
            across(piece, theirs, m).wait_recv()
            within(piece, mine2, m).start()
        for piece, m, _ in pieces(k - 2):
            within(piece, theirs2, m).wait_recv()

    def ag(i):
        for k in range(7):
            c = i - k
            if isinstance(c, int):
                if 0 <= c < chunks:
                    ag_chunk(jnp.int32(c), k)
            else:
                @pl.when(jnp.logical_and(c >= 0, c < chunks))
                def _(c=c, k=k):
                    ag_chunk(c, k)

    def rs_chunk(c, k):
        s = 1 - 2 * (c % 2)
        a_to, b_to = {"dp": at_z(s)}, {"dp": at_z(-s)}

        def send_a(src, m):
            return remote(src, ra.at[c, m], rs.at[c, m], rr.at[c, m], a_to)

        def send_b(src, m):
            return remote(src, rb.at[c, m], rs.at[c, 4 + m], rr.at[c, 4 + m], b_to)

        def add(ref, dest):
            ref[...] = (ref[...].astype(F32) + g[c, dest].astype(F32)).astype(BF16)

        if k == 0:
            send_a(g.at[c, at_z(4 * s)], 0).start()
        if k == 1:
            send_b(g.at[c, at_z(-3 * s)], 0).start()
        if 1 <= k <= 3:
            send_a(ra.at[c, k - 1], k - 1).wait_recv()
            add(ra.at[c, k - 1], at_z((4 - k) * s))
            send_a(ra.at[c, k - 1], k).start()
        if 2 <= k <= 3:
            send_b(rb.at[c, k - 2], k - 2).wait_recv()
            add(rb.at[c, k - 2], at_z(-(4 - k) * s))
            send_b(rb.at[c, k - 2], k - 1).start()
        if k == 4:
            send_a(ra.at[c, 3], 3).wait_recv()
            send_b(rb.at[c, 2], 2).wait_recv()
            out[c] = (g[c, me].astype(F32) + ra[c, 3].astype(F32) + rb[c, 2].astype(F32)).astype(BF16)

    def rs_step(i, first=0):
        for k in (3, 2, 1, 0, 4):
            if k < first:
                continue

            @pl.when(jnp.logical_and(i - k >= 0, i - k < chunks))
            def _(k=k):
                rs_chunk(chunk_at(i - k), k)

    def chunk_at(i):
        return jnp.where(i < blocks, i + (layers - 1) * blocks, i - blocks) if layers == 2 else i

    def over_tiles(body):
        def one(t, _):
            body(pl.ds(pl.multiple_of(t * tile, tile), tile))
            return 0
        lax.fori_loop(0, tiles, one, 0)

    def norm(src, with_t):
        def body(r):
            wide = src[r, :].astype(F32)
            scale = lax.rsqrt(jnp.mean(wide * wide, -1, keepdims=True) + 1e-6)
            normed = (wide * scale).astype(BF16)
            a[r, :] = normed
            acc[r, :] = jnp.zeros((tile, width), F32)
            if with_t:
                at[:, r] = normed.T
        over_tiles(body)

    def transpose_d():
        def body(r):
            dt[:, r] = d[r, :].T
        over_tiles(body)

    def forward_block(c):
        def body(r):
            gu = dot(a[r, :], w[c, :, :tall, :].reshape(width, width))
            gate, up = gu[:, :fb], gu[:, fb:]
            sig = 0.5 * jnp.tanh(0.5 * gate) + 0.5
            prod = (gate * sig * up).astype(BF16)
            acc[r, :] += dot(prod, w[c, :, tall:, :].reshape(fb, width))
        over_tiles(body)

    def backward_block(c):
        def body(r):
            wgu = w[c, :, :tall, :].reshape(width, width)
            gu = dot(a[r, :], wgu)
            dh = dot(d[r, :], w[c, :, tall:, :].reshape(fb, width), NT)
            gate, up = gu[:, :fb], gu[:, fb:]
            sig = 0.5 * jnp.tanh(0.5 * gate) + 0.5
            silu = gate * sig
            hid[r, :] = (silu * up).astype(BF16)
            dgu[r, fb:] = (dh * silu).astype(BF16)
            dgu[r, :fb] = (dh * up * (sig + silu * (1.0 - sig))).astype(BF16)
            acc[r, :] += dot(dgu[r, :], wgu, NT)
        over_tiles(body)
        g[c, :, :tall, :] = dot(at[...], dgu[...]).astype(BF16).reshape(n, tall, width)
        g[c, :, tall:, :] = dot(dt[...], hid[...]).T.astype(BF16).reshape(n, rows - tall, width)

    def norm_back(src, dst):
        def body(r):
            wide = src[r, :].astype(F32)
            scale = lax.rsqrt(jnp.mean(wide * wide, -1, keepdims=True) + 1e-6)
            da = acc[r, :]
            mix = jnp.mean(da * wide, -1, keepdims=True) * scale * scale
            dst[r, :] = (d[r, :].astype(F32) + scale * (da - wide * mix)).astype(BF16)
        over_tiles(body)

    ag(0)
    get_x.wait()
    ag(1)
    norm(x, False)
    get_d.wait()
    ag(2)
    transpose_d()
    for i in range(3, 7):
        ag(i)

    def fwd(j, _):
        forward_block(j)
        ag(j + 7)
        return 0
    lax.fori_loop(0, blocks, fwd, 0)

    def to_h(r):
        h[r, :] = (x[r, :].astype(F32) + acc[r, :].astype(BF16).astype(F32)).astype(BF16)
    over_tiles(to_h)
    norm(h, True)

    def bwd2(j, _):
        backward_block(j + blocks)
        rs_step(j)
        ag(j + 7 + blocks)
        return 0
    lax.fori_loop(0, blocks, bwd2, 0)

    norm_back(h, d)
    transpose_d()
    norm(x, True)

    def bwd1(j, _):
        backward_block(j)
        rs_step(j + blocks)
        return 0
    lax.fori_loop(0, blocks, bwd1, 0)

    norm_back(x, a)
    put_dx = pltpu.make_async_copy(a, dx_hbm, local.at[0])
    put_dx.start()

    def drain(i, _):
        rs_step(i, 1)
        return 0
    lax.fori_loop(chunks, chunks + 4, drain, 0)
    put_out = pltpu.make_async_copy(out, out_hbm, local.at[1])
    put_out.start()

    def sent(c, _):
        for m in range(7):
            q = w.at[c, 0, :, pl.ds(0, quarter)]
            remote(q, q, zs.at[c, m], zr.at[c, m], {"dp": at_z(1)}).wait_send()
            remote(q, q, xs.at[c, m], xr.at[c, m], {"dp": at_z(1)}).wait_send()
            q = w.at[c, 0, :, pl.ds(0, half)]
            remote(q, q, cs.at[c, m], cr.at[c, m], {"dp": at_z(1)}).wait_send()
            q = g.at[c, 0]
            remote(q, q, rs.at[c, m], rr.at[c, m], {"dp": at_z(1)}).wait_send()
        return 0
    lax.fori_loop(0, chunks, sent, 0)
    put_dx.wait()
    put_out.wait()


def solution(mesh):
    n = mesh.shape["dp"]
    near, far = chips_apart(mesh)

    def on_device(x, dy, wg, wu, wd):
        x, dy = x[0], dy[0]
        tokens, width = x.shape
        layers, tall, ff = wg.shape
        fb = width // 2
        blocks = ff // fb
        sub = fb // n
        rows = tall + sub
        chunks = layers * blocks
        tile = min(512, tokens)

        def cut(w):
            return w.reshape(layers, tall, n, blocks, sub).transpose(0, 3, 1, 2, 4).reshape(layers, blocks, tall, fb)

        wp = jnp.concatenate([cut(wg), cut(wu)], -1)
        wp = jnp.concatenate([wp, wd.reshape(layers, blocks, sub, width)], 2).reshape(chunks, rows, width)
        anywhere = pl.BlockSpec(memory_space=pl.ANY)
        dma = pltpu.SemaphoreType.DMA((chunks, 7))
        dx, out = pl.pallas_call(
            functools.partial(kernel, (n, near, far, tile, layers)),
            out_shape=(jax.ShapeDtypeStruct((tokens, width), BF16),
                       jax.ShapeDtypeStruct((chunks, rows, width), BF16)),
            in_specs=[anywhere] * 3,
            out_specs=(anywhere, anywhere),
            scratch_shapes=[
                pltpu.VMEM((tokens, width), BF16),
                pltpu.VMEM((tokens, width), BF16),
                pltpu.VMEM((tokens, width), BF16),
                pltpu.VMEM((tokens, width), BF16),
                pltpu.VMEM((width, tokens), BF16),
                pltpu.VMEM((width, tokens), BF16),
                pltpu.VMEM((tokens, width), F32),
                pltpu.VMEM((tokens, width), BF16),
                pltpu.VMEM((tokens, fb), BF16),
                pltpu.VMEM((chunks, n, rows, width), BF16),
                pltpu.VMEM((chunks, n, rows, width), BF16),
                pltpu.VMEM((chunks, 4, rows, width), BF16),
                pltpu.VMEM((chunks, 3, rows, width), BF16),
                pltpu.VMEM((chunks, rows, width), BF16),
                dma, dma, dma, dma, dma, dma, dma, dma,
                pltpu.SemaphoreType.DMA((3,)),
            ],
            compiler_params=pltpu.CompilerParams(
                collective_id=0, has_side_effects=True, vmem_limit_bytes=67_043_328),
        )(x, dy, wp)
        out = out.reshape(layers, blocks, rows, width)

        def whole(part):
            part = part.reshape(layers, blocks, tall, n, sub).transpose(0, 2, 3, 1, 4)
            return part.reshape(layers, tall, ff)

        return (dx[None], whole(out[:, :, :tall, :fb]), whole(out[:, :, :tall, fb:]),
                out[:, :, tall:, :].reshape(layers, blocks * sub, width))

    tokens_spec, w_spec = P(("rep", "dp"), None, None), P(None, "dp", None)
    return jax.shard_map(
        on_device, mesh=mesh,
        in_specs=(tokens_spec, tokens_spec, w_spec, w_spec, w_spec),
        out_specs=(tokens_spec, P("rep", "dp", None), P("rep", "dp", None), P("rep", "dp", None)),
        check_vma=False)
```

```python
import functools

import jax
import jax.numpy as jnp
from jax import lax
from jax.experimental import pallas as pl
from jax.experimental.pallas import tpu as pltpu
from jax.sharding import PartitionSpec as P

MESH = pl.DeviceIdType.MESH
F32, BF16 = jnp.float32, jnp.bfloat16
NN = (((1,), (0,)), ((), ()))
NT = (((1,), (1,)), ((), ()))
GAP, STAGES = 4, 7


def dot(a, b, dims=NN):
    return lax.dot_general(a, b, dims, preferred_element_type=F32)


def chips_apart(mesh):
    first = mesh.devices.reshape(mesh.shape["rep"], -1)[:, 0]
    places = [getattr(d, "coords", None) for d in first]
    if places[0] is None:
        return 2, 4
    near = 2
    far = next((i for i, p in enumerate(places) if p[0] != places[0][0]), 4)
    return near, far


def kernel(cfg, x_hbm, dy_hbm, wg_hbm, wu_hbm, wd_hbm, dx_hbm, og_hbm, ou_hbm, od_hbm,
           x, d, h, a1, at1, a2, at2, dt, acc, dgu, hid, wgs, wus, w, g, ra, rb, out,
           zs, zr, xs, xr, cs, cr, rs, rr, local):
    n, near, far, tile, layers = cfg
    tokens, width = x.shape
    chunks, _, rows, _ = w.shape
    blocks = chunks // layers
    tall = width // n
    fb = width // 2
    sub = fb // n
    quarter, half = width // 4, width // 2
    tiles = tokens // tile
    cut = rows // 2
    later = blocks - 1

    me, rep = lax.axis_index("dp"), lax.axis_index("rep")
    core, ybit, xbit = rep % 2, (rep // near) % 2, (rep // far) % 2
    other_core = rep + 1 - 2 * core
    other_y = rep + near * (1 - 2 * ybit)
    other_x = rep + far * (1 - 2 * xbit)

    def at_z(k):
        return lax.rem(me + k + 2 * n, n)

    barrier = pltpu.get_barrier_semaphore()
    for who in ({"dp": at_z(1)}, {"dp": at_z(-1)}, {"rep": other_core}, {"rep": other_y}, {"rep": other_x}):
        pl.semaphore_signal(barrier, inc=1, device_id=who, device_id_type=MESH)
    loads = [
        pltpu.make_async_copy(wg_hbm, wgs, local.at[0]),
        pltpu.make_async_copy(wu_hbm, wus, local.at[1]),
        pltpu.make_async_copy(wd_hbm, w.at[:, me, tall:, :], local.at[2]),
    ]
    get_x = pltpu.make_async_copy(x_hbm, x, local.at[3])
    get_d = pltpu.make_async_copy(dy_hbm, d, local.at[4])
    for copy in (*loads, get_x, get_d):
        copy.start()
    for copy in loads:
        copy.wait()

    def prepare(c):
        l, j = divmod(c, blocks)
        ff = sub * blocks
        parts = [src[l, :, o * ff + j * sub:o * ff + (j + 1) * sub] for src in (wgs, wus) for o in range(n)]
        w[c, me, :tall, :] = jnp.concatenate(parts, -1)

    def remote(src, dst, ssem, rsem, who):
        return pltpu.make_async_remote_copy(
            src_ref=src, dst_ref=dst, send_sem=ssem, recv_sem=rsem, device_id=who, device_id_type=MESH)

    def ag_chunk(c, k):
        par = c % 2
        s = 1 - 2 * par
        bit = ybit + par * (xbit - ybit)
        partner = other_y + par * (other_x - other_y)
        mine = pl.ds(pl.multiple_of((2 * core + bit) * quarter, quarter), quarter)
        theirs = pl.ds(pl.multiple_of((2 * core + 1 - bit) * quarter, quarter), quarter)
        mine2 = pl.ds(pl.multiple_of(core * half, half), half)
        theirs2 = pl.ds(pl.multiple_of((1 - core) * half, half), half)
        a_to, b_to = {"dp": at_z(s)}, {"dp": at_z(-s)}

        def hop(who, piece, m):
            ref = w.at[c, piece, :, mine]
            return remote(ref, ref, zs.at[c, m], zr.at[c, m], who)

        def across(piece, cols, m):
            ref = w.at[c, piece, :, cols]
            return remote(ref, ref, xs.at[c, m], xr.at[c, m], {"rep": partner})

        def within(piece, cols, m):
            ref = w.at[c, piece, :, cols]
            return remote(ref, ref, cs.at[c, m], cr.at[c, m], {"rep": other_core})

        def pieces(j):
            found = []
            if 1 <= j <= 4:
                found.append((at_z(-j * s), j - 1, a_to if j < 4 else None))
            if 1 <= j <= 3:
                found.append((at_z(j * s), 4 + j - 1, b_to if j < 3 else None))
            return found

        if k == 0:
            hop(a_to, me, 0).start()
            hop(b_to, me, 4).start()
        for piece, m, on in pieces(k):
            hop(a_to, piece, m).wait_recv()
            if on is not None:
                hop(on, piece, m + 1).start()
            across(piece, mine, m).start()
        for piece, m, _ in pieces(k - 1):
            across(piece, theirs, m).wait_recv()
            within(piece, mine2, m).start()
        for piece, m, _ in pieces(k - 2):
            within(piece, theirs2, m).wait_recv()

    def ag(i, first, gap):
        for k in range(STAGES - 1, -1, -1):
            c = i - gap * k
            if isinstance(c, int):
                if 0 <= c < blocks:
                    ag_chunk(jnp.int32(first + c), k)
            else:
                @pl.when(jnp.logical_and(c >= 0, c < blocks))
                def _(c=c, k=k):
                    ag_chunk(first + c, k)

    ag1 = functools.partial(ag, first=0, gap=GAP)
    ag2 = functools.partial(ag, first=blocks, gap=1)
    startup = GAP * (STAGES - 1)
    early = STAGES - (blocks + 1) // 2

    def rs_chunk(c, k):
        a_to, b_to = {"dp": at_z(1)}, {"dp": at_z(-1)}
        top, low = pl.ds(0, cut), pl.ds(cut, cut)

        def send_a(src, dst, m):
            return remote(src, dst, rs.at[c, m], rr.at[c, m], a_to)

        def send_b(src, dst, m):
            return remote(src, dst, rs.at[c, 4 + m], rr.at[c, 4 + m], b_to)

        def add(ref, dest, part):
            ref[part, :] = (ref[part, :].astype(F32) + g[c, dest, part, :].astype(F32)).astype(BF16)

        everything = pl.ds(0, rows)
        if k == 0:
            send_a(g.at[c, at_z(4), top], ra.at[c, 0, top], 0).start()
            send_b(g.at[c, at_z(-4), low], rb.at[c, 0, low], 0).start()
        if k == 1:
            ra[c, 0, low, :] = g[c, at_z(3), low, :]
            rb[c, 0, top, :] = g[c, at_z(-3), top, :]
            send_a(ra.at[c, 0, top], ra.at[c, 0, top], 0).wait_recv()
            add(ra.at[c, 0], at_z(3), top)
            send_a(ra.at[c, 0], ra.at[c, 1], 1).start()
            send_b(rb.at[c, 0, low], rb.at[c, 0, low], 0).wait_recv()
            add(rb.at[c, 0], at_z(-3), low)
            send_b(rb.at[c, 0], rb.at[c, 1], 1).start()
        if k in (2, 3):
            send_a(ra.at[c, k - 1], ra.at[c, k - 1], k - 1).wait_recv()
            add(ra.at[c, k - 1], at_z(4 - k), everything)
            send_a(ra.at[c, k - 1], ra.at[c, k], k).start()
            send_b(rb.at[c, k - 1], rb.at[c, k - 1], k - 1).wait_recv()
            add(rb.at[c, k - 1], at_z(k - 4), everything)
            send_b(rb.at[c, k - 1], rb.at[c, k], k).start()
        if k == 4:
            send_a(ra.at[c, 3], ra.at[c, 3], 3).wait_recv()
            send_b(rb.at[c, 3], rb.at[c, 3], 3).wait_recv()
            out[c] = (g[c, me].astype(F32) + ra[c, 3].astype(F32) + rb[c, 3].astype(F32)).astype(BF16)

    def chunk_at(i):
        return lax.rem(i + (layers - 1) * blocks, chunks)

    def rs_do(i, k):
        @pl.when(jnp.logical_and(i - k >= 0, i - k < chunks))
        def _():
            rs_chunk(chunk_at(i - k), k)

    def over_tiles(body, between=None):
        def one(t, _):
            if between is not None:
                between(t)
            body(pl.ds(pl.multiple_of(t * tile, tile), tile))
            return 0
        lax.fori_loop(0, tiles, one, 0)

    def put_normed(wide, r, a, at):
        scale = lax.rsqrt(jnp.mean(wide * wide, -1, keepdims=True) + 1e-6)
        normed = (wide * scale).astype(BF16)
        a[r, :] = normed
        at[:, r] = normed.T

    def first_norm():
        def body(r):
            put_normed(x[r, :].astype(F32), r, a1, at1)
            acc[r, :] = jnp.zeros((tile, width), F32)
        over_tiles(body)

    def transpose_d():
        def body(r):
            dt[:, r] = d[r, :].T
        over_tiles(body)

    def next_state():
        def body(r):
            new = (x[r, :].astype(F32) + acc[r, :].astype(BF16).astype(F32)).astype(BF16)
            h[r, :] = new
            put_normed(new.astype(F32), r, a2, at2)
            acc[r, :] = jnp.zeros((tile, width), F32)
        over_tiles(body)

    def forward_block(c, between):
        def body(r):
            gu = dot(a1[r, :], w[c, :, :tall, :].reshape(width, width))
            gate, up = gu[:, :fb], gu[:, fb:]
            sig = 0.5 * jnp.tanh(0.5 * gate) + 0.5
            prod = (gate * sig * up).astype(BF16)
            acc[r, :] += dot(prod, w[c, :, tall:, :].reshape(fb, width))
        over_tiles(body, between)

    def backward_block(c, a, at, between, after):
        def body(r):
            wgu = w[c, :, :tall, :].reshape(width, width)
            gu = dot(a[r, :], wgu)
            dh = dot(d[r, :], w[c, :, tall:, :].reshape(fb, width), NT)
            gate, up = gu[:, :fb], gu[:, fb:]
            sig = 0.5 * jnp.tanh(0.5 * gate) + 0.5
            silu = gate * sig
            hid[r, :] = (silu * up).astype(BF16)
            dgu[r, fb:] = (dh * silu).astype(BF16)
            dgu[r, :fb] = (dh * up * (sig + silu * (1.0 - sig))).astype(BF16)
            acc[r, :] += dot(dgu[r, :], wgu, NT)
        over_tiles(body, between)
        after()
        g[c, :, :tall, :] = dot(at[...], dgu[...]).astype(BF16).reshape(n, tall, width)
        g[c, :, tall:, :] = dot(dt[...], hid[...]).T.astype(BF16).reshape(n, rows - tall, width)

    def norm_back(src, dst, last):
        def body(r):
            wide = src[r, :].astype(F32)
            scale = lax.rsqrt(jnp.mean(wide * wide, -1, keepdims=True) + 1e-6)
            da = acc[r, :]
            mix = jnp.mean(da * wide, -1, keepdims=True) * scale * scale
            new = (d[r, :].astype(F32) + scale * (da - wide * mix)).astype(BF16)
            dst[r, :] = new
            if not last:
                dt[:, r] = new.T
                acc[r, :] = jnp.zeros((tile, width), F32)
        over_tiles(body)

    prepare(0)
    pl.semaphore_wait(barrier, 5)
    for i in range(startup + 1):
        ag1(i)
        if i + 1 < chunks:
            prepare(i + 1)
        if i == blocks:
            get_x.wait()
            first_norm()
        if i == blocks + GAP:
            get_d.wait()
            transpose_d()
        q = early - 1 - (startup - 2 - i) // 4
        if (startup - 2 - i) % 4 == 0 and 0 <= q < early:
            ag2(q)

    def fwd(j, _):
        def between(t):
            for m in range(2):
                @pl.when(t == m * tiles // 2)
                def _():
                    ag1(startup + 1 + 2 * j + m)

            @pl.when(jnp.logical_and(t == tiles - 1, j % 2 == 0))
            def _():
                ag2(early + j // 2)
        forward_block(j, between)
        return 0
    lax.fori_loop(0, blocks, fwd, 0)
    next_state()

    def rs_between(i):
        def between(t):
            for m in range(3):
                @pl.when(t == m * tiles // 4)
                def _():
                    rs_do(i, 4 - m)
        return between

    def bwd2(j, _):
        backward_block(j + blocks, a2, at2, rs_between(j), lambda: rs_do(j, 1))
        rs_do(j, 0)
        ag2(STAGES + j)
        return 0
    lax.fori_loop(0, blocks, bwd2, 0)

    norm_back(h, d, False)

    def bwd1(j, _):
        backward_block(j, a1, at1, rs_between(j + blocks), lambda: rs_do(j + blocks, 1))
        rs_do(j + blocks, 0)
        return 0
    lax.fori_loop(0, blocks, bwd1, 0)

    norm_back(x, a2, True)
    put_dx = pltpu.make_async_copy(a2, dx_hbm, local.at[0])
    put_dx.start()

    def drain(i, _):
        for k in (3, 2, 1, 4):
            rs_do(i, k)
        return 0

    def put_out(l, at):
        blocks_of = pl.ds(l * blocks, blocks)
        for which, dst in enumerate((wgs, wus)):
            dst[l] = jnp.concatenate(
                [out[l * blocks + j, :tall, which * fb + o * sub:which * fb + (o + 1) * sub]
                 for o in range(n) for j in range(blocks)], -1)
        return [pltpu.make_async_copy(out.at[blocks_of, tall:, :], od_hbm.at[blocks_of], local.at[at]),
                pltpu.make_async_copy(wgs.at[l], og_hbm.at[l], local.at[at + 1]),
                pltpu.make_async_copy(wus.at[l], ou_hbm.at[l], local.at[at + 2])]

    def gathers_sent(c, _):
        for m in range(7):
            q = w.at[c, 0, :, pl.ds(0, quarter)]
            remote(q, q, zs.at[c, m], zr.at[c, m], {"dp": at_z(1)}).wait_send()
            remote(q, q, xs.at[c, m], xr.at[c, m], {"dp": at_z(1)}).wait_send()
            q = w.at[c, 0, :, pl.ds(0, half)]
            remote(q, q, cs.at[c, m], cr.at[c, m], {"dp": at_z(1)}).wait_send()
        return 0

    def sums_sent(c, _):
        for m in range(8):
            q = g.at[c, 0, pl.ds(0, cut)] if m % 4 == 0 else g.at[c, 0]
            remote(q, q, rs.at[c, m], rr.at[c, m], {"dp": at_z(1)}).wait_send()
        return 0

    lax.fori_loop(chunks, chunks + 1, drain, 0)
    puts = []
    for l in range(1, layers):
        puts += put_out(l, 3 * l + 1)
    for copy in puts:
        copy.start()
    lax.fori_loop(0, chunks, gathers_sent, 0)
    lax.fori_loop(chunks + 1, chunks + 4, drain, 0)
    last = put_out(0, 1)
    for copy in last:
        copy.start()
    lax.fori_loop(0, chunks, sums_sent, 0)
    for copy in (put_dx, *puts, *last):
        copy.wait()


def handed_on(*arrays):
    pieces = [(i, k) for i, a in enumerate(arrays) for k in range(4 if i == 0 else 1)]

    def body(*refs):
        src, dst = refs[:len(arrays)], refs[len(arrays):2 * len(arrays)]
        here, sems = refs[2 * len(arrays):3 * len(arrays)], refs[-1]

        def part(ref, i, k):
            if i:
                return ref
            rows = ref.shape[0] // 4
            return ref.at[pl.ds(k * rows, rows)]

        into = [pltpu.make_async_copy(part(src[i], i, k), part(here[i], i, k), sems.at[0, m])
                for m, (i, k) in enumerate(pieces)]
        back = [pltpu.make_async_copy(part(here[i], i, k), part(dst[i], i, k), sems.at[1, m])
                for m, (i, k) in enumerate(pieces)]
        for copy in into:
            copy.start()
        for one, two in zip(into, back):
            one.wait()
            two.start()
        for copy in back:
            copy.wait()

    anywhere = pl.BlockSpec(memory_space=pl.ANY)
    return pl.pallas_call(
        body,
        out_shape=tuple(jax.ShapeDtypeStruct(a.shape, a.dtype) for a in arrays),
        in_specs=[anywhere] * len(arrays),
        out_specs=(anywhere,) * len(arrays),
        scratch_shapes=[*(pltpu.VMEM(a.shape, a.dtype) for a in arrays),
                        pltpu.SemaphoreType.DMA((2, len(pieces)))],
    )(*arrays)


def solution(mesh):
    n = mesh.shape["dp"]
    near, far = chips_apart(mesh)

    def on_device(x, dy, wg, wu, wd):
        x, dy = x[0], dy[0]
        tokens, width = x.shape
        layers, tall, ff = wg.shape
        fb = width // 2
        blocks = ff // fb
        sub = fb // n
        rows = tall + sub
        chunks = layers * blocks
        tile = min(1024, tokens // 2)
        anywhere = pl.BlockSpec(memory_space=pl.ANY)
        seven, eight = pltpu.SemaphoreType.DMA((chunks, 7)), pltpu.SemaphoreType.DMA((chunks, 8))
        wide, high = pltpu.VMEM((tokens, width), BF16), pltpu.VMEM((width, tokens), BF16)
        dx, og, ou, od = pl.pallas_call(
            functools.partial(kernel, (n, near, far, tile, layers)),
            out_shape=(jax.ShapeDtypeStruct(x.shape, BF16),
                       jax.ShapeDtypeStruct(wg.shape, BF16),
                       jax.ShapeDtypeStruct(wu.shape, BF16),
                       jax.ShapeDtypeStruct((chunks, sub, width), BF16)),
            in_specs=[anywhere] * 5,
            out_specs=(anywhere,) * 4,
            scratch_shapes=[
                wide, wide, wide, wide, high, wide, high, high,
                pltpu.VMEM((tokens, width), F32),
                wide,
                pltpu.VMEM((tokens, fb), BF16),
                pltpu.VMEM(wg.shape, BF16),
                pltpu.VMEM(wu.shape, BF16),
                pltpu.VMEM((chunks, n, rows, width), BF16),
                pltpu.VMEM((chunks, n, rows, width), BF16),
                pltpu.VMEM((chunks, 4, rows, width), BF16),
                pltpu.VMEM((chunks, 4, rows, width), BF16),
                pltpu.VMEM((chunks, rows, width), BF16),
                seven, seven, seven, seven, seven, seven, eight, eight,
                pltpu.SemaphoreType.DMA((7,)),
            ],
            compiler_params=pltpu.CompilerParams(
                collective_id=0, has_side_effects=True, vmem_limit_bytes=67_043_328),
        )(x, dy, wg, wu, wd.reshape(chunks, sub, width))
        dx, og, ou, od = handed_on(dx, og, ou, od)
        return dx[None], og, ou, od.reshape(wd.shape)

    tokens_spec, w_spec = P(("rep", "dp"), None, None), P(None, "dp", None)
    return jax.shard_map(
        on_device, mesh=mesh,
        in_specs=(tokens_spec, tokens_spec, w_spec, w_spec, w_spec),
        out_specs=(tokens_spec, P("rep", "dp", None), P("rep", "dp", None), P("rep", "dp", None)),
        check_vma=False)
```

```python
import functools

import jax
import jax.numpy as jnp
from jax import lax
from jax.experimental import pallas as pl
from jax.experimental.pallas import tpu as pltpu
from jax.sharding import PartitionSpec as P

MESH = pl.DeviceIdType.MESH
F32, BF16 = jnp.float32, jnp.bfloat16
NN = (((1,), (0,)), ((), ()))
NT = (((1,), (1,)), ((), ()))
GAP, STAGES = 4, 7


def dot(a, b, dims=NN):
    return lax.dot_general(a, b, dims, preferred_element_type=F32)


def chips_apart(mesh):
    first = mesh.devices.reshape(mesh.shape["rep"], -1)[:, 0]
    places = [getattr(d, "coords", None) for d in first]
    if places[0] is None:
        return 2, 4
    near = 2
    far = next((i for i, p in enumerate(places) if p[0] != places[0][0]), 4)
    return near, far


def kernel(cfg, x_hbm, dy_hbm, wg_hbm, wu_hbm, wd_hbm, dx_hbm, og_hbm, ou_hbm, od_hbm,
           x, d, h, a1, at1, a2, at2, dt, acc, dgu, hid, wgs, wus, w, g, ra, rb, out,
           zs, zr, xs, xr, cs, cr, rs, rr, local):
    n, near, far, tile, layers = cfg
    tokens, width = x.shape
    chunks, _, rows, _ = w.shape
    blocks = chunks // layers
    tall = width // n
    fb = width // 2
    sub = fb // n
    quarter, half = width // 4, width // 2
    tiles = tokens // tile
    cut = rows // 2
    later = blocks - 1

    me, rep = lax.axis_index("dp"), lax.axis_index("rep")
    core, ybit, xbit = rep % 2, (rep // near) % 2, (rep // far) % 2
    other_core = rep + 1 - 2 * core
    other_y = rep + near * (1 - 2 * ybit)
    other_x = rep + far * (1 - 2 * xbit)

    def at_z(k):
        return lax.rem(me + k + 2 * n, n)

    barrier = pltpu.get_barrier_semaphore()
    for who in ({"dp": at_z(1)}, {"dp": at_z(-1)}, {"rep": other_core}, {"rep": other_y}, {"rep": other_x}):
        pl.semaphore_signal(barrier, inc=1, device_id=who, device_id_type=MESH)
    loads = [
        pltpu.make_async_copy(wg_hbm, wgs, local.at[0]),
        pltpu.make_async_copy(wu_hbm, wus, local.at[1]),
        pltpu.make_async_copy(wd_hbm, w.at[:, me, tall:, :], local.at[2]),
    ]
    get_x = pltpu.make_async_copy(x_hbm, x, local.at[3])
    get_d = pltpu.make_async_copy(dy_hbm, d, local.at[4])
    for copy in (*loads, get_x, get_d):
        copy.start()
    for copy in loads:
        copy.wait()

    def prepare(c):
        l, j = divmod(c, blocks)
        ff = sub * blocks
        parts = [src[l, :, o * ff + j * sub:o * ff + (j + 1) * sub] for src in (wgs, wus) for o in range(n)]
        w[c, me, :tall, :] = jnp.concatenate(parts, -1)

    def remote(src, dst, ssem, rsem, who):
        return pltpu.make_async_remote_copy(
            src_ref=src, dst_ref=dst, send_sem=ssem, recv_sem=rsem, device_id=who, device_id_type=MESH)

    def ag_chunk(c, k):
        par = c % 2
        s = 1 - 2 * par
        bit = ybit + par * (xbit - ybit)
        partner = other_y + par * (other_x - other_y)
        mine = pl.ds(pl.multiple_of((2 * core + bit) * quarter, quarter), quarter)
        theirs = pl.ds(pl.multiple_of((2 * core + 1 - bit) * quarter, quarter), quarter)
        mine2 = pl.ds(pl.multiple_of(core * half, half), half)
        theirs2 = pl.ds(pl.multiple_of((1 - core) * half, half), half)
        a_to, b_to = {"dp": at_z(s)}, {"dp": at_z(-s)}

        def hop(who, piece, m):
            ref = w.at[c, piece, :, mine]
            return remote(ref, ref, zs.at[c, m], zr.at[c, m], who)

        def across(piece, cols, m):
            ref = w.at[c, piece, :, cols]
            return remote(ref, ref, xs.at[c, m], xr.at[c, m], {"rep": partner})

        def within(piece, cols, m):
            ref = w.at[c, piece, :, cols]
            return remote(ref, ref, cs.at[c, m], cr.at[c, m], {"rep": other_core})

        def pieces(j):
            found = []
            if 1 <= j <= 4:
                found.append((at_z(-j * s), j - 1, a_to if j < 4 else None))
            if 1 <= j <= 3:
                found.append((at_z(j * s), 4 + j - 1, b_to if j < 3 else None))
            return found

        if k == 0:
            hop(a_to, me, 0).start()
            hop(b_to, me, 4).start()
        for piece, m, on in pieces(k):
            hop(a_to, piece, m).wait_recv()
            if on is not None:
                hop(on, piece, m + 1).start()
            across(piece, mine, m).start()
        for piece, m, _ in pieces(k - 1):
            across(piece, theirs, m).wait_recv()
            within(piece, mine2, m).start()
        for piece, m, _ in pieces(k - 2):
            within(piece, theirs2, m).wait_recv()

    def ag(i, first, gap):
        for k in range(STAGES - 1, -1, -1):
            c = i - gap * k
            if isinstance(c, int):
                if 0 <= c < blocks:
                    ag_chunk(jnp.int32(first + c), k)
            else:
                @pl.when(jnp.logical_and(c >= 0, c < blocks))
                def _(c=c, k=k):
                    ag_chunk(first + c, k)

    ag1 = functools.partial(ag, first=0, gap=GAP)
    ag2 = functools.partial(ag, first=blocks, gap=1)
    startup = GAP * (STAGES - 1)
    early = STAGES - (blocks + 1) // 2

    def rs_chunk(c, k):
        a_to, b_to = {"dp": at_z(1)}, {"dp": at_z(-1)}
        top, low = pl.ds(0, cut), pl.ds(cut, cut)

        def send_a(src, dst, m):
            return remote(src, dst, rs.at[c, m], rr.at[c, m], a_to)

        def send_b(src, dst, m):
            return remote(src, dst, rs.at[c, 4 + m], rr.at[c, 4 + m], b_to)

        def add(ref, dest, part):
            ref[part, :] = (ref[part, :].astype(F32) + g[c, dest, part, :].astype(F32)).astype(BF16)

        everything = pl.ds(0, rows)
        if k == 0:
            send_a(g.at[c, at_z(4), top], ra.at[c, 0, top], 0).start()
            send_b(g.at[c, at_z(-4), low], rb.at[c, 0, low], 0).start()
        if k == 1:
            ra[c, 0, low, :] = g[c, at_z(3), low, :]
            rb[c, 0, top, :] = g[c, at_z(-3), top, :]
            send_a(ra.at[c, 0, top], ra.at[c, 0, top], 0).wait_recv()
            add(ra.at[c, 0], at_z(3), top)
            send_a(ra.at[c, 0], ra.at[c, 1], 1).start()
            send_b(rb.at[c, 0, low], rb.at[c, 0, low], 0).wait_recv()
            add(rb.at[c, 0], at_z(-3), low)
            send_b(rb.at[c, 0], rb.at[c, 1], 1).start()
        if k in (2, 3):
            send_a(ra.at[c, k - 1], ra.at[c, k - 1], k - 1).wait_recv()
            add(ra.at[c, k - 1], at_z(4 - k), everything)
            send_a(ra.at[c, k - 1], ra.at[c, k], k).start()
            send_b(rb.at[c, k - 1], rb.at[c, k - 1], k - 1).wait_recv()
            add(rb.at[c, k - 1], at_z(k - 4), everything)
            send_b(rb.at[c, k - 1], rb.at[c, k], k).start()
        if k == 4:
            send_a(ra.at[c, 3], ra.at[c, 3], 3).wait_recv()
            send_b(rb.at[c, 3], rb.at[c, 3], 3).wait_recv()
            out[c] = (g[c, me].astype(F32) + ra[c, 3].astype(F32) + rb[c, 3].astype(F32)).astype(BF16)

    def chunk_at(i):
        return lax.rem(i + (layers - 1) * blocks, chunks)

    def rs_do(i, k):
        @pl.when(jnp.logical_and(i - k >= 0, i - k < chunks))
        def _():
            rs_chunk(chunk_at(i - k), k)

    def over_tiles(body, between=None):
        def one(t, _):
            if between is not None:
                between(t)
            body(pl.ds(pl.multiple_of(t * tile, tile), tile))
            return 0
        lax.fori_loop(0, tiles, one, 0)

    def put_normed(wide, r, a, at):
        scale = lax.rsqrt(jnp.mean(wide * wide, -1, keepdims=True) + 1e-6)
        normed = (wide * scale).astype(BF16)
        a[r, :] = normed
        at[:, r] = normed.T

    def first_norm():
        def body(r):
            put_normed(x[r, :].astype(F32), r, a1, at1)
            acc[r, :] = jnp.zeros((tile, width), F32)
        over_tiles(body)

    def transpose_d():
        def body(r):
            dt[:, r] = d[r, :].T
        over_tiles(body)

    def next_state():
        def body(r):
            new = (x[r, :].astype(F32) + acc[r, :].astype(BF16).astype(F32)).astype(BF16)
            h[r, :] = new
            put_normed(new.astype(F32), r, a2, at2)
            acc[r, :] = jnp.zeros((tile, width), F32)
        over_tiles(body)

    def forward_block(c, between):
        def body(r):
            gu = dot(a1[r, :], w[c, :, :tall, :].reshape(width, width))
            gate, up = gu[:, :fb], gu[:, fb:]
            sig = 0.5 * jnp.tanh(0.5 * gate) + 0.5
            prod = (gate * sig * up).astype(BF16)
            acc[r, :] += dot(prod, w[c, :, tall:, :].reshape(fb, width))
        over_tiles(body, between)

    def backward_block(c, a, at, between, after):
        def body(r):
            wgu = w[c, :, :tall, :].reshape(width, width)
            gu = dot(a[r, :], wgu)
            dh = dot(d[r, :], w[c, :, tall:, :].reshape(fb, width), NT)
            gate, up = gu[:, :fb], gu[:, fb:]
            sig = 0.5 * jnp.tanh(0.5 * gate) + 0.5
            silu = gate * sig
            hid[r, :] = (silu * up).astype(BF16)
            dgu[r, fb:] = (dh * silu).astype(BF16)
            dgu[r, :fb] = (dh * up * (sig + silu * (1.0 - sig))).astype(BF16)
            acc[r, :] += dot(dgu[r, :], wgu, NT)
        over_tiles(body, between)
        after()
        g[c, :, :tall, :] = dot(at[...], dgu[...]).astype(BF16).reshape(n, tall, width)
        g[c, :, tall:, :] = dot(dt[...], hid[...]).T.astype(BF16).reshape(n, rows - tall, width)

    def norm_back(src, dst, last, between):
        def body(r):
            wide = src[r, :].astype(F32)
            scale = lax.rsqrt(jnp.mean(wide * wide, -1, keepdims=True) + 1e-6)
            da = acc[r, :]
            mix = jnp.mean(da * wide, -1, keepdims=True) * scale * scale
            new = (d[r, :].astype(F32) + scale * (da - wide * mix)).astype(BF16)
            dst[r, :] = new
            if not last:
                dt[:, r] = new.T
                acc[r, :] = jnp.zeros((tile, width), F32)
        over_tiles(body, between)

    prepare(0)
    pl.semaphore_wait(barrier, 5)
    for i in range(startup + 1):
        ag1(i)
        if i + 1 < chunks:
            prepare(i + 1)
        if i == blocks:
            get_x.wait()
            first_norm()
        if i == blocks + GAP:
            get_d.wait()
            transpose_d()
        q = early - 1 - (startup - 2 - i) // 4
        if (startup - 2 - i) % 4 == 0 and 0 <= q < early:
            ag2(q)

    def fwd(j, _):
        def between(t):
            @pl.when(t == tiles // 2)
            def _():
                ag1(startup + 1 + 2 * j)
        forward_block(j, between)
        ag1(startup + 2 + 2 * j)

        @pl.when(j % 2 == 0)
        def _():
            ag2(early + j // 2)
        return 0
    lax.fori_loop(0, blocks, fwd, 0)
    next_state()

    def rs_between(i):
        def between(t):
            @pl.when(jnp.logical_and(t == 0, i != blocks))
            def _():
                rs_do(i, 4)
                rs_do(i, 3)

            @pl.when(t == tiles // 2)
            def _():
                rs_do(i, 2)
        return between

    def rs_halves(i, ks):
        def between(t):
            for m, k in enumerate(ks):
                @pl.when(t == m * tiles // 2)
                def _():
                    rs_do(jnp.int32(i), k)
        return between

    def bwd2(j, _):
        backward_block(j + blocks, a2, at2, rs_between(j), lambda: rs_do(j, 1))
        rs_do(j, 0)
        ag2(STAGES + j)
        return 0
    lax.fori_loop(0, blocks, bwd2, 0)

    norm_back(h, d, False, rs_halves(blocks, (4, 3)))

    def bwd1(j, _):
        backward_block(j, a1, at1, rs_between(j + blocks), lambda: rs_do(j + blocks, 1))
        rs_do(j + blocks, 0)
        return 0
    lax.fori_loop(0, blocks, bwd1, 0)

    norm_back(x, a2, True, rs_halves(chunks, (3, 2)))
    put_dx = pltpu.make_async_copy(a2, dx_hbm, local.at[0])
    put_dx.start()

    def drain(i, _):
        for k in (3, 2, 1, 4):
            rs_do(i, k)
        return 0

    def put_out(l, at):
        blocks_of = pl.ds(l * blocks, blocks)
        for which, dst in enumerate((wgs, wus)):
            dst[l] = jnp.concatenate(
                [out[l * blocks + j, :tall, which * fb + o * sub:which * fb + (o + 1) * sub]
                 for o in range(n) for j in range(blocks)], -1)
        return [pltpu.make_async_copy(out.at[blocks_of, tall:, :], od_hbm.at[blocks_of], local.at[at]),
                pltpu.make_async_copy(wgs.at[l], og_hbm.at[l], local.at[at + 1]),
                pltpu.make_async_copy(wus.at[l], ou_hbm.at[l], local.at[at + 2])]

    def gathers_sent(c, _):
        for m in range(7):
            q = w.at[c, 0, :, pl.ds(0, quarter)]
            remote(q, q, zs.at[c, m], zr.at[c, m], {"dp": at_z(1)}).wait_send()
            remote(q, q, xs.at[c, m], xr.at[c, m], {"dp": at_z(1)}).wait_send()
            q = w.at[c, 0, :, pl.ds(0, half)]
            remote(q, q, cs.at[c, m], cr.at[c, m], {"dp": at_z(1)}).wait_send()
        return 0

    def sums_sent(c, _):
        for m in range(8):
            q = g.at[c, 0, pl.ds(0, cut)] if m % 4 == 0 else g.at[c, 0]
            remote(q, q, rs.at[c, m], rr.at[c, m], {"dp": at_z(1)}).wait_send()
        return 0

    for k in (1, 4):
        rs_do(jnp.int32(chunks), k)
    puts = []
    for l in range(1, layers):
        puts += put_out(l, 3 * l + 1)
    for copy in puts:
        copy.start()
    lax.fori_loop(0, chunks, gathers_sent, 0)
    lax.fori_loop(chunks + 1, chunks + 4, drain, 0)
    last = put_out(0, 1)
    for copy in last:
        copy.start()
    lax.fori_loop(0, chunks, sums_sent, 0)
    for copy in (put_dx, *puts, *last):
        copy.wait()


def handed_on(*arrays):
    pieces = [(i, k) for i, a in enumerate(arrays) for k in range(4 if i == 0 else 1)]

    def body(*refs):
        src, dst = refs[:len(arrays)], refs[len(arrays):2 * len(arrays)]
        here, sems = refs[2 * len(arrays):3 * len(arrays)], refs[-1]

        def part(ref, i, k):
            if i:
                return ref
            rows = ref.shape[0] // 4
            return ref.at[pl.ds(k * rows, rows)]

        into = [pltpu.make_async_copy(part(src[i], i, k), part(here[i], i, k), sems.at[0, m])
                for m, (i, k) in enumerate(pieces)]
        back = [pltpu.make_async_copy(part(here[i], i, k), part(dst[i], i, k), sems.at[1, m])
                for m, (i, k) in enumerate(pieces)]
        for copy in into:
            copy.start()
        for one, two in zip(into, back):
            one.wait()
            two.start()
        for copy in back:
            copy.wait()

    anywhere = pl.BlockSpec(memory_space=pl.ANY)
    return pl.pallas_call(
        body,
        out_shape=tuple(jax.ShapeDtypeStruct(a.shape, a.dtype) for a in arrays),
        in_specs=[anywhere] * len(arrays),
        out_specs=(anywhere,) * len(arrays),
        scratch_shapes=[*(pltpu.VMEM(a.shape, a.dtype) for a in arrays),
                        pltpu.SemaphoreType.DMA((2, len(pieces)))],
    )(*arrays)


def solution(mesh):
    n = mesh.shape["dp"]
    near, far = chips_apart(mesh)

    def on_device(x, dy, wg, wu, wd):
        x, dy = x[0], dy[0]
        tokens, width = x.shape
        layers, tall, ff = wg.shape
        fb = width // 2
        blocks = ff // fb
        sub = fb // n
        rows = tall + sub
        chunks = layers * blocks
        tile = min(1024, tokens // 2)
        anywhere = pl.BlockSpec(memory_space=pl.ANY)
        seven, eight = pltpu.SemaphoreType.DMA((chunks, 7)), pltpu.SemaphoreType.DMA((chunks, 8))
        wide, high = pltpu.VMEM((tokens, width), BF16), pltpu.VMEM((width, tokens), BF16)
        dx, og, ou, od = pl.pallas_call(
            functools.partial(kernel, (n, near, far, tile, layers)),
            out_shape=(jax.ShapeDtypeStruct(x.shape, BF16),
                       jax.ShapeDtypeStruct(wg.shape, BF16),
                       jax.ShapeDtypeStruct(wu.shape, BF16),
                       jax.ShapeDtypeStruct((chunks, sub, width), BF16)),
            in_specs=[anywhere] * 5,
            out_specs=(anywhere,) * 4,
            scratch_shapes=[
                wide, wide, wide, wide, high, wide, high, high,
                pltpu.VMEM((tokens, width), F32),
                wide,
                pltpu.VMEM((tokens, fb), BF16),
                pltpu.VMEM(wg.shape, BF16),
                pltpu.VMEM(wu.shape, BF16),
                pltpu.VMEM((chunks, n, rows, width), BF16),
                pltpu.VMEM((chunks, n, rows, width), BF16),
                pltpu.VMEM((chunks, 4, rows, width), BF16),
                pltpu.VMEM((chunks, 4, rows, width), BF16),
                pltpu.VMEM((chunks, rows, width), BF16),
                seven, seven, seven, seven, seven, seven, eight, eight,
                pltpu.SemaphoreType.DMA((7,)),
            ],
            compiler_params=pltpu.CompilerParams(
                collective_id=0, has_side_effects=True, vmem_limit_bytes=67_043_328),
        )(x, dy, wg, wu, wd.reshape(chunks, sub, width))
        dx, og, ou, od = handed_on(dx, og, ou, od)
        return dx[None], og, ou, od.reshape(wd.shape)

    tokens_spec, w_spec = P(("rep", "dp"), None, None), P(None, "dp", None)
    return jax.shard_map(
        on_device, mesh=mesh,
        in_specs=(tokens_spec, tokens_spec, w_spec, w_spec, w_spec),
        out_specs=(tokens_spec, P("rep", "dp", None), P("rep", "dp", None), P("rep", "dp", None)),
        check_vma=False)
```
